32 devices in a mesh: gx: 4 (over x, core), gy: 2 (over y), gz: 4 (over z).
Axes of the slice: x: 2, y: 2, z: 4, core: 2. Of those that a mesh axis runs over, the one named last changes fastest.
Arguments:
- velocity_rhs: float32 [3, 32, 32, 512], P(None, 'gz', 'gy', 'gx'), may hold values from -48 to 48
- pressure_rhs: float32 [16, 16, 256], P('gz', 'gy', 'gx'), may hold values from -6 to 6
- viscosity: float32 [32, 32, 512], P('gz', 'gy', 'gx'), may hold values from 0.6 to 1.4
- velocity_mass: float32 [32, 32, 512], P('gz', 'gy', 'gx'), may hold values from 0.5 to 4
- pressure_scale: float32 [16, 16, 256], P('gz', 'gy', 'gx'), may hold values from 0.6 to 1.5
- velocity_bounds: float32 [2], replicated, may hold values from 4 to 72, as said below
- pressure_bounds: float32 [2], replicated, may hold values from 0.08 to 2.8, as said below
Outputs:
- velocity: float32 [3, 32, 32, 512], P(None, 'gz', 'gy', 'gx')
- pressure: float32 [16, 16, 256], P('gz', 'gy', 'gx')
The draws below stay inside these ranges and needn't reach their ends.
Inputs may be any that keep to these rules, and one draw needn't show every extreme that they name: velocity_bounds[0] is the lower bound and velocity_bounds[1] the upper one; the upper one exceeds the largest eigenvalue of A. pressure_bounds[0] is the lower bound and pressure_bounds[1] the upper one; the upper one exceeds the largest eigenvalue of M.
All inputs are finite; a program needn't handle non-finite values.
Results may differ from the reference program's by a relative error of at most 0.00002.
Values sent between devices are 32-bit elements; how exact they have to be, the bound alone decides.
A program may use at most 64 MiB of HBM per device.

```python
import math
import jax
import jax.numpy as jnp
from jax import lax

SWEEPS = 2
PITERS = 2
NX = 512
NY = 32
NZ = 32
PX = 256
PY = 16
PZ = 16


def draw_velocity_bounds(key, part):
    values = jax.random.uniform(jax.random.fold_in(key, 11), (2,), jnp.float32)
    return jnp.stack([4.0 + 6.0 * values[0], 62.0 + 10.0 * values[1]]).astype(jnp.float32)


def draw_pressure_bounds(key, part):
    values = jax.random.uniform(jax.random.fold_in(key, 23), (2,), jnp.float32)
    return jnp.stack([0.08 + 0.22 * values[0], 2.4 + 0.4 * values[1]]).astype(jnp.float32)


def levels(key, shape, cuts, smallest, top_value):
    level, own = 1.0, jax.random.fold_in(key, 6)
    for axis_at, blocks in cuts:
        draws = jnp.exp(jax.random.uniform(jax.random.fold_in(own, axis_at), (blocks,), jnp.float32, smallest / len(cuts), top_value / len(cuts)))
        level = level * jnp.repeat(draws, shape[axis_at] // blocks).reshape([-1 if axis == axis_at else 1 for axis in range(len(shape))])
    return level


def centred(key, extent, scale, bound, split=(), kind=jnp.bfloat16):
    gain = levels(key, extent, split, -0.22, 0.18) if split else 1.0
    entries = jax.random.normal(key, extent, jnp.float32) * scale * gain
    return jnp.minimum(jnp.maximum(entries, -bound), bound).astype(kind)


def setup_inputs(seed: int = 0) -> dict:
    key_of = jax.random.split(jax.random.key(seed), 8)
    velocity_rhs = centred(key_of[0], (3, NZ, NY, NX), 8.0, 48.0, ((1, 4), (2, 2), (3, 4)), jnp.float32)
    pressure_rhs = centred(key_of[1], (PZ, PY, PX), 1.0, 6.0, ((0, 4), (1, 2), (2, 4)), jnp.float32)
    viscosity = jnp.clip(jnp.exp(math.log(1.4) - 0.8472978 * jax.random.uniform(key_of[2], (NZ, NY, NX), jnp.float32) ** levels(key_of[2], (NZ, NY, NX), ((0, 4), (1, 2), (2, 4)), -0.2, 0.2)), 0.6, 1.4)
    velocity_mass = jnp.clip(jnp.exp(math.log(4.0) - 2.0794415 * jax.random.uniform(key_of[3], (NZ, NY, NX), jnp.float32) ** levels(key_of[3], (NZ, NY, NX), ((0, 4), (1, 2), (2, 4)), -0.2, 0.2)), 0.5, 4.0)
    pressure_scale = jnp.clip(jnp.exp(math.log(1.5) - 0.9162907 * jax.random.uniform(key_of[4], (PZ, PY, PX), jnp.float32) ** levels(key_of[4], (PZ, PY, PX), ((0, 4), (1, 2), (2, 4)), -0.2, 0.2)), 0.6, 1.5)
    velocity_bounds = draw_velocity_bounds(jax.random.fold_in(key_of[7], 71), 0)
    pressure_bounds = draw_pressure_bounds(jax.random.fold_in(key_of[7], 71), 0)
    return {"velocity_rhs": velocity_rhs, "pressure_rhs": pressure_rhs, "viscosity": viscosity, "velocity_mass": velocity_mass, "pressure_scale": pressure_scale, "velocity_bounds": velocity_bounds, "pressure_bounds": pressure_bounds}


def pad_cells(field, width):
    return jnp.pad(field, [(0, 0)] * (field.ndim - 3) + [(width, width)] * 3)


def smooth_three(padded, outer_weight, centre):
    result = padded
    base = padded.ndim - 3
    for offset in range(3):
        dimension = base + offset
        length = result.shape[dimension] - 2
        result = (outer_weight * lax.slice_in_dim(result, 0, length, axis=dimension)
                  + centre * lax.slice_in_dim(result, 1, length + 1, axis=dimension)
                  + outer_weight * lax.slice_in_dim(result, 2, length + 2, axis=dimension))
    return result


def chebyshev(source, operator, bounds, count):
    low_end = bounds[0]
    high_end = bounds[1]
    centre_value = (high_end + low_end) / 2.0
    spread = (high_end - low_end) / 2.0
    sigma_ratio = centre_value / spread
    factor = 1.0 / sigma_ratio
    direction = source / centre_value
    iterate = direction
    residual = source
    for repeat in range(count):
        residual = residual - operator(direction)
        factor_next = 1.0 / (2.0 * sigma_ratio - factor)
        direction = factor_next * factor * direction + (2.0 * factor_next / spread) * residual
        iterate = iterate + direction
        factor = factor_next
    return iterate


def restrict_one(field, dimension):
    count = (field.shape[dimension] - 2) // 2
    return (0.25 * lax.slice_in_dim(field, 0, 2 * count, stride=2, axis=dimension)
            + 0.5 * lax.slice_in_dim(field, 1, 2 * count + 1, stride=2, axis=dimension)
            + 0.25 * lax.slice_in_dim(field, 2, 2 * count + 2, stride=2, axis=dimension))


def divergence_restricted(padded):
    along_x = 0.5 * (padded[0, 1:-1, 1:-1, 2:] - padded[0, 1:-1, 1:-1, :-2])
    along_y = 0.5 * (padded[1, 1:-1, 2:, 1:-1] - padded[1, 1:-1, :-2, 1:-1])
    along_z = 0.5 * (padded[2, 2:, 1:-1, 1:-1] - padded[2, :-2, 1:-1, 1:-1])
    diverge = along_x + along_y + along_z
    for dimension in range(3):
        diverge = restrict_one(diverge, dimension)
    return diverge


def reference(velocity_rhs, pressure_rhs, viscosity, velocity_mass, pressure_scale, velocity_bounds, pressure_bounds):
    def apply_velocity(direction):
        weighted = viscosity * direction
        laplace = 16.0 * weighted - 2.0 * smooth_three(pad_cells(weighted, 1), 0.5, 1.0)
        return viscosity * laplace + velocity_mass * direction

    def smooth_component(component):
        return chebyshev(component, apply_velocity, velocity_bounds, SWEEPS)

    velocity = lax.map(smooth_component, velocity_rhs)
    coupled = pressure_rhs - divergence_restricted(pad_cells(velocity, 2))

    def apply_pressure(direction):
        weighted = pressure_scale * direction
        return pressure_scale * smooth_three(pad_cells(weighted, 1), 1.0 / 6.0, 2.0 / 3.0)

    pressure = chebyshev(coupled, apply_pressure, pressure_bounds, PITERS)
    return velocity, pressure
```

```python
import itertools

import jax
import jax.numpy as jnp
from jax import lax
from jax.experimental import pallas as pl
from jax.experimental.pallas import tpu as pltpu
from jax.sharding import PartitionSpec as P

SWEEPS = 2
PITERS = 2
BELOW = SWEEPS + 2
ABOVE = SWEEPS + 1
ROWS = 8
FIELDS = 5
GROUP = 8
MESH = pl.DeviceIdType.MESH
AXES = ("gx", "gy", "gz")
DIRECTIONS = [d for d in itertools.product((0, -1, 1), repeat=3) if d != (0, 0, 0)]
DIRECTIONS.sort(key=lambda d: -sum(abs(c) for c in d))


def chebyshev_scalars(bounds, count):
    low, high = bounds[0], bounds[1]
    theta = (high + low) * 0.5
    delta = (high - low) * 0.5
    sigma = theta / delta
    rho = 1.0 / sigma
    steps = []
    for _ in range(count):
        rho_next = 1.0 / (2.0 * sigma - rho)
        steps.append((rho_next * rho, 2.0 * rho_next / delta))
        rho = rho_next
    return 1.0 / theta, steps


def average(value, axis, outer, centre):
    size = value.shape[axis]
    return centre * value + outer * (pltpu.roll(value, 1, axis) + pltpu.roll(value, size - 1, axis))


def kernel(
    vrhs, prhs, visc, mass, pscale, vbounds, pbounds,
    vout, pout,
    main, left, right, packed,
    wide_b, wide_v, wide_m, smooth, smooth_next, resid, direct, total,
    gathered, prhs_in, pscale_in, scale_all, coupled_all, to_pressure, rows_at, vres, pres,
    local_sem, send_sem, recv_sem,
):
    nz, ny, nx = visc.shape
    pz, py, px = pscale.shape
    depth = BELOW + nz + ABOVE
    sizes = [lax.axis_size(a) for a in AXES]
    at = [lax.axis_index(a) for a in AXES]

    def exists(d):
        ok = None
        for coordinate, place, size in zip(d, at, sizes):
            if coordinate:
                here = place > 0 if coordinate < 0 else place < size - 1
                ok = here if ok is None else jnp.logical_and(ok, here)
        return ok

    def target(d):
        return {a: p + c for a, p, c in zip(AXES, at, d)}

    mid = pl.ds(BELOW, nz)
    loads = [
        pltpu.make_async_copy(vrhs, main.at[pl.ds(0, 3), mid, pl.ds(0, ny), :], local_sem.at[0]),
        pltpu.make_async_copy(visc, main.at[3, mid, pl.ds(0, ny), :], local_sem.at[1]),
        pltpu.make_async_copy(mass, main.at[4, mid, pl.ds(0, ny), :], local_sem.at[2]),
        pltpu.make_async_copy(pscale, pscale_in, local_sem.at[3]),
        pltpu.make_async_copy(prhs, prhs_in, local_sem.at[4]),
    ]
    for load in loads:
        load.start()

    for f in range(FIELDS):
        main[f, pl.ds(0, BELOW)] = jnp.zeros((BELOW, ny + 2 * ROWS, nx), jnp.float32)
        main[f, pl.ds(BELOW + nz, ABOVE)] = jnp.zeros((ABOVE, ny + 2 * ROWS, nx), jnp.float32)
        main[f, mid, pl.ds(ny, 2 * ROWS)] = jnp.zeros((nz, 2 * ROWS, nx), jnp.float32)
    left[...] = jnp.zeros_like(left)
    right[...] = jnp.zeros_like(right)
    scale_all[...] = jnp.zeros_like(scale_all)
    coupled_all[...] = jnp.zeros_like(coupled_all)

    barrier = pltpu.get_barrier_semaphore()
    count = None
    for place, size in zip(at, sizes):
        span = 1 + jnp.where(place > 0, 1, 0) + jnp.where(place < size - 1, 1, 0)
        count = span if count is None else count * span
    for d in DIRECTIONS:
        @pl.when(exists(d))
        def _(d=d):
            pl.semaphore_signal(barrier, inc=1, device_id=target(d), device_id_type=MESH)

    x_at = lax.broadcasted_iota(jnp.int32, (2 * nx, 2 * px), 0)
    x_at = jnp.where(x_at < nx + nx // 2, x_at, x_at - 2 * nx)
    column = lax.broadcasted_iota(jnp.int32, (2 * nx, 2 * px), 1)
    offset = x_at - 2 * jnp.where(column < px, column, column - px)
    apart = jnp.where(offset < 0, -offset, offset)
    to_pressure[0] = jnp.where(apart == 0, 0.5, jnp.where(apart == 1, 0.25, 0.0))
    slope = jnp.where(apart == 1, 0.25, jnp.where(apart == 2, 0.125, 0.0))
    to_pressure[1] = jnp.where(offset < 0, -slope, slope)

    for load in loads:
        load.wait()

    lane = lax.broadcasted_iota(jnp.int32, (ny, nx), 1)

    @pl.loop(0, nz)
    def _(k):
        edge = main[0, BELOW + k, pl.ds(0, ny), :]
        for f in range(1, FIELDS):
            moved = pltpu.roll(main[f, BELOW + k, pl.ds(0, ny), :], GROUP * f, 1)
            inside = jnp.logical_and(lane >= GROUP * f - BELOW, lane < GROUP * f + BELOW)
            edge = jnp.where(inside, moved, edge)
        packed[k] = edge

    scale_own = pscale_in[...]
    scale_all[1, pl.ds(PITERS, pz), pl.ds(0, py), :] = jnp.concatenate([scale_own, scale_own], axis=2)

    pl.semaphore_wait(barrier, count - 1)

    def velocity_copy(d):
        dx, dy, dz = d
        z_from, z_to, z_many = {
            0: (BELOW, BELOW, nz), 1: (nz, 0, BELOW), -1: (BELOW, BELOW + nz, ABOVE)}[dz]
        y_from, y_to, y_many = {
            0: (0, 0, ny), 1: (ny - ROWS, ny + ROWS, ROWS), -1: (0, ny, ROWS)}[dy]
        if dx == 0:
            source = main.at[:, pl.ds(z_from, z_many), pl.ds(y_from, y_many), :]
            place = main.at[:, pl.ds(z_to, z_many), pl.ds(y_to, y_many), :]
        else:
            source = packed.at[pl.ds(z_from - BELOW, z_many), pl.ds(y_from, y_many), :]
            place = (left if dx == 1 else right).at[pl.ds(z_to, z_many), pl.ds(y_to, y_many), :]
        at_sem = DIRECTIONS.index(d)
        return pltpu.make_async_remote_copy(
            src_ref=source, dst_ref=place, send_sem=send_sem.at[0, at_sem],
            recv_sem=recv_sem.at[0, at_sem], device_id=target(d), device_id_type=MESH)

    def pressure_copy(buffer, which, d):
        dx, dy, dz = d
        z_from, z_to, z_many = {
            0: (PITERS, PITERS, pz), 1: (pz, 0, PITERS), -1: (PITERS, PITERS + pz, PITERS)}[dz]
        y_to = {0: 0, 1: 2 * ROWS, -1: ROWS}[dy]
        at_sem = DIRECTIONS.index(d)
        return pltpu.make_async_remote_copy(
            src_ref=buffer.at[1, pl.ds(z_from, z_many), pl.ds(0, ROWS), :],
            dst_ref=buffer.at[1 - dx, pl.ds(z_to, z_many), pl.ds(y_to, ROWS), :],
            send_sem=send_sem.at[which, at_sem], recv_sem=recv_sem.at[which, at_sem],
            device_id=target(d), device_id_type=MESH)

    def opposite(d):
        return tuple(-c for c in d)

    for d in DIRECTIONS:
        @pl.when(exists(d))
        def _(d=d):
            velocity_copy(d).start()
            pressure_copy(scale_all, 1, d).start()

    start_v, steps_v = chebyshev_scalars(vbounds, SWEEPS)
    start_p, steps_p = chebyshev_scalars(pbounds, PITERS)

    for d in DIRECTIONS:
        @pl.when(exists(opposite(d)))
        def _(d=d):
            velocity_copy(d).wait_recv()
            pressure_copy(scale_all, 1, d).wait_recv()

    row8 = lax.broadcasted_iota(jnp.int32, (ROWS, nx), 0) < ROWS // 2
    wide_lane = lax.broadcasted_iota(jnp.int32, (ny + ROWS, nx), 1)
    from_right = lax.rem(wide_lane, GROUP) < GROUP // 2

    def fold_rows(block):
        low, up, down = block[:-2 * ROWS], block[-2 * ROWS:-ROWS], block[-ROWS:]
        return jnp.concatenate([low, jnp.where(row8[:, :block.shape[1]], up, down)], axis=0)

    @pl.loop(0, depth)
    def _(k):
        halo = jnp.where(from_right, fold_rows(right[k]), fold_rows(left[k]))

        def whole(f):
            side = pltpu.roll(halo, nx - GROUP * f, 1) if f else halo
            return jnp.concatenate([fold_rows(main[f, k]), side], axis=1)

        weight = whole(3)
        wide_v[k] = weight
        wide_m[k] = whole(4)
        for c in range(3):
            source = whole(c)
            wide_b[c, k] = source
            smooth[c, k] = average(average(weight * (source * start_v), 1, 0.5, 1.0), 0, 0.5, 1.0)

    def apply_wide(c, k, held, direction, weight):
        mean = held[c, k] + 0.5 * (held[c, k - 1] + held[c, k + 1])
        return weight * (16.0 * (weight * direction) - 2.0 * mean) + wide_m[k] * direction

    @pl.loop(1, depth - 1)
    def _(k):
        weight = wide_v[k]
        for c in range(3):
            source = wide_b[c, k]
            first = source * start_v
            rest = source - apply_wide(c, k, smooth, first, weight)
            second = steps_v[0][0] * first + steps_v[0][1] * rest
            resid[c, k] = rest
            direct[c, k] = second
            total[c, k] = first + second
            smooth_next[c, k] = average(average(weight * second, 1, 0.5, 1.0), 0, 0.5, 1.0)

    @pl.loop(2, depth - 2)
    def _(k):
        weight = wide_v[k]
        for c in range(3):
            second = direct[c, k]
            rest = resid[c, k] - apply_wide(c, k, smooth_next, second, weight)
            total[c, k] = total[c, k] + (steps_v[1][0] * second + steps_v[1][1] * rest)

    for c in range(3):
        vres[c] = total[c, mid, pl.ds(0, ny), pl.ds(0, nx)]
    store_velocity = pltpu.make_async_copy(vres, vout, local_sem.at[5])
    store_velocity.start()

    for k in range(pz):
        z = BELOW + 2 * k
        for c in range(2):
            gathered[c, k] = 0.5 * total[c, z] + 0.25 * (total[c, z - 1] + total[c, z + 1])
        gathered[2, k] = 0.25 * (total[2, z + 1] - total[2, z - 1]) + 0.125 * (
            total[2, z + 2] - total[2, z - 2])
    wide_rows = ny + ROWS

    def along_x(c, matrix):
        return jnp.dot(
            gathered[c].reshape(pz * wide_rows, 2 * nx), to_pressure[matrix],
            precision=lax.Precision.HIGHEST, preferred_element_type=jnp.float32,
        ).reshape(pz, wide_rows, 2 * px)

    part0, part1, part2 = along_x(0, 1), along_x(1, 0), along_x(2, 0)
    for k in range(pz):
        u = part1[k]
        one = pltpu.roll(u, wide_rows - 1, 0) - pltpu.roll(u, 1, 0)
        two = pltpu.roll(u, wide_rows - 2, 0) - pltpu.roll(u, 2, 0)
        rows_at[k] = average(part0[k] + part2[k], 0, 0.25, 0.5) + (0.25 * one + 0.125 * two)
    for k in range(pz):
        source = prhs_in[k]
        coupled_all[1, PITERS + k, pl.ds(0, py), :] = (
            jnp.concatenate([source, source], axis=1) - rows_at[k, pl.ds(0, py, stride=2), :])

    for d in DIRECTIONS:
        @pl.when(exists(d))
        def _(d=d):
            pressure_copy(coupled_all, 2, d).start()

    for d in DIRECTIONS:
        @pl.when(exists(opposite(d)))
        def _(d=d):
            pressure_copy(coupled_all, 2, d).wait_recv()

    narrow_lane = lax.broadcasted_iota(jnp.int32, (py + ROWS, 2 * px), 1)
    deep = pz + 2 * PITERS

    def whole_pressure(buffer, k):
        outside = jnp.where(
            narrow_lane < px + px // 2, fold_rows(buffer[2, k]), fold_rows(buffer[0, k]))
        return jnp.where(narrow_lane < px, fold_rows(buffer[1, k]), outside)

    scales = [whole_pressure(scale_all, k) for k in range(deep)]
    rest = [whole_pressure(coupled_all, k) for k in range(deep)]
    way = [value * start_p for value in rest]
    answer = list(way)
    for n in range(PITERS):
        mean = [
            average(average(scales[k] * way[k], 1, 1 / 6, 2 / 3), 0, 1 / 6, 2 / 3) if n <= k < deep - n else None
            for k in range(deep)]
        for k in range(n + 1, deep - n - 1):
            applied = scales[k] * ((2 / 3) * mean[k] + (1 / 6) * (mean[k - 1] + mean[k + 1]))
            rest[k] = rest[k] - applied
            way[k] = steps_p[n][0] * way[k] + steps_p[n][1] * rest[k]
            answer[k] = answer[k] + way[k]
    for k in range(pz):
        pres[k] = answer[PITERS + k][:py, :px]
    store_pressure = pltpu.make_async_copy(pres, pout, local_sem.at[6])
    store_pressure.start()

    for d in DIRECTIONS:
        @pl.when(exists(d))
        def _(d=d):
            velocity_copy(d).wait_send()
            pressure_copy(scale_all, 1, d).wait_send()
            pressure_copy(coupled_all, 2, d).wait_send()
    store_velocity.wait()
    store_pressure.wait()


def per_device(vrhs, prhs, visc, mass, pscale, vbounds, pbounds):
    nz, ny, nx = visc.shape
    pz, py, px = pscale.shape
    depth = BELOW + nz + ABOVE
    wide = (depth, ny + ROWS, 2 * nx)
    f32 = jnp.float32
    anywhere = pl.BlockSpec(memory_space=pl.ANY)
    scalars = pl.BlockSpec(memory_space=pltpu.SMEM)
    ways = len(DIRECTIONS)
    edge = (depth, ny + 2 * ROWS, nx)
    pressure_all = (3, pz + 2 * PITERS, py + 2 * ROWS, 2 * px)
    return pl.pallas_call(
        kernel,
        out_shape=(jax.ShapeDtypeStruct(vrhs.shape, f32), jax.ShapeDtypeStruct(prhs.shape, f32)),
        in_specs=[anywhere] * 5 + [scalars] * 2,
        out_specs=(anywhere, anywhere),
        scratch_shapes=[
            pltpu.VMEM((FIELDS,) + edge, f32),
            pltpu.VMEM(edge, f32),
            pltpu.VMEM(edge, f32),
            pltpu.VMEM((nz, ny, nx), f32),
            pltpu.VMEM((3,) + wide, f32),
            pltpu.VMEM(wide, f32),
            pltpu.VMEM(wide, f32),
            pltpu.VMEM((3,) + wide, f32),
            pltpu.VMEM((3,) + wide, f32),
            pltpu.VMEM((3,) + wide, f32),
            pltpu.VMEM((3,) + wide, f32),
            pltpu.VMEM((3,) + wide, f32),
            pltpu.VMEM((3, pz, ny + ROWS, 2 * nx), f32),
            pltpu.VMEM((pz, py, px), f32),
            pltpu.VMEM((pz, py, px), f32),
            pltpu.VMEM(pressure_all, f32),
            pltpu.VMEM(pressure_all, f32),
            pltpu.VMEM((2, 2 * nx, 2 * px), f32),
            pltpu.VMEM((pz, ny + ROWS, 2 * px), f32),
            pltpu.VMEM((3, nz, ny, nx), f32),
            pltpu.VMEM((pz, py, px), f32),
            pltpu.SemaphoreType.DMA((7,)),
            pltpu.SemaphoreType.DMA((3, ways)),
            pltpu.SemaphoreType.DMA((3, ways)),
        ],
        compiler_params=pltpu.CompilerParams(collective_id=0, has_side_effects=True),
    )(vrhs, prhs, visc, mass, pscale, vbounds, pbounds)


def solution(mesh):
    cells = P("gz", "gy", "gx")
    in_specs = (P(None, "gz", "gy", "gx"), cells, cells, cells, cells, P(), P())
    out_specs = (P(None, "gz", "gy", "gx"), cells)
    return jax.shard_map(
        per_device, mesh=mesh, in_specs=in_specs, out_specs=out_specs, check_vma=False
    )
```

```python
import itertools

import jax
import jax.numpy as jnp
from jax import lax
from jax.experimental import pallas as pl
from jax.experimental.pallas import tpu as pltpu
from jax.sharding import PartitionSpec as P

SWEEPS = 2
PITERS = 2
BELOW = SWEEPS + 2
ABOVE = SWEEPS + 1
ROWS = 8
FIELDS = 5
VISCOSITY, MASS, COMPONENT = 1, 4, (2, 3, 0)
DEEP = 2
GROUP = 8
MESH = pl.DeviceIdType.MESH
AXES = ("gx", "gy", "gz")
DIRECTIONS = [d for d in itertools.product((0, -1, 1), repeat=3) if d != (0, 0, 0)]
DIRECTIONS.sort(key=lambda d: -sum(abs(c) for c in d))


def chebyshev_scalars(bounds, count):
    low, high = bounds[0], bounds[1]
    theta = (high + low) * 0.5
    delta = (high - low) * 0.5
    sigma = theta / delta
    rho = 1.0 / sigma
    steps = []
    for _ in range(count):
        rho_next = 1.0 / (2.0 * sigma - rho)
        steps.append((rho_next * rho, 2.0 * rho_next / delta))
        rho = rho_next
    return 1.0 / theta, steps


def average(value, axis, outer, centre):
    size = value.shape[axis]
    return centre * value + outer * (pltpu.roll(value, 1, axis) + pltpu.roll(value, size - 1, axis))


def kernel(
    vrhs, prhs, visc, mass, pscale, vbounds, pbounds,
    vout, pout,
    main, left, right, packed, ysend, yrecv,
    wide_b, wide_v, wide_m, smooth, smooth_next, resid, direct, total,
    gathered, prhs_in, pscale_in, scale_all, coupled_all, to_pressure, rows_at, vres, pres,
    local_sem, send_sem, recv_sem,
):
    nz, ny, nx = visc.shape
    pz, py, px = pscale.shape
    depth = BELOW + nz + ABOVE
    sizes = [lax.axis_size(a) for a in AXES]
    at = [lax.axis_index(a) for a in AXES]

    def exists(d):
        ok = None
        for coordinate, place, size in zip(d, at, sizes):
            if coordinate:
                here = place > 0 if coordinate < 0 else place < size - 1
                ok = here if ok is None else jnp.logical_and(ok, here)
        return ok

    def target(d):
        return {a: p + c for a, p, c in zip(AXES, at, d)}

    mid = pl.ds(BELOW, nz)
    loads = [
        pltpu.make_async_copy(vrhs.at[pl.ds(0, 2)], main.at[pl.ds(2, 2), mid], local_sem.at[0]),
        pltpu.make_async_copy(vrhs.at[2], main.at[0, mid], local_sem.at[7]),
        pltpu.make_async_copy(visc, main.at[VISCOSITY, mid], local_sem.at[1]),
        pltpu.make_async_copy(mass, main.at[MASS, mid], local_sem.at[2]),
        pltpu.make_async_copy(pscale, pscale_in, local_sem.at[3]),
        pltpu.make_async_copy(prhs, prhs_in, local_sem.at[4]),
    ]
    for load in loads:
        load.start()

    barrier = pltpu.get_barrier_semaphore()
    count = None
    for place, size in zip(at, sizes):
        span = 1 + jnp.where(place > 0, 1, 0) + jnp.where(place < size - 1, 1, 0)
        count = span if count is None else count * span
    for d in DIRECTIONS:
        @pl.when(exists(d))
        def _(d=d):
            pl.semaphore_signal(barrier, inc=1, device_id=target(d), device_id_type=MESH)

    def clear(*refs):
        for ref in refs:
            ref[...] = jnp.zeros(ref.shape, jnp.float32)

    for plane in (0, depth - 1):
        for f in range(DEEP, FIELDS):
            clear(main.at[f, plane])
        for side in range(2):
            for t in range(1, 3):
                clear(yrecv.at[side, t, plane])

    def missing(axis, sign):
        return at[axis] == (0 if sign < 0 else sizes[axis] - 1)

    for sign, buffer, slot in ((-1, left, 0), (1, right, 2)):
        @pl.when(missing(0, sign))
        def _(buffer=buffer, slot=slot):
            clear(buffer, scale_all.at[slot], coupled_all.at[slot])

    for sign, side in ((1, 0), (-1, 1)):
        @pl.when(missing(1, sign))
        def _(side=side):
            rows = pl.ds(ny + side * ROWS, ROWS)
            clear(yrecv.at[side], left.at[:, rows], right.at[:, rows])
            rows = pl.ds(py + side * ROWS, ROWS)
            clear(scale_all.at[:, :, rows], coupled_all.at[:, :, rows])

    for sign, place, many, pplace in ((-1, 0, BELOW, 0), (1, BELOW + nz, ABOVE, PITERS + pz)):
        @pl.when(missing(2, sign))
        def _(place=place, many=many, pplace=pplace):
            planes = pl.ds(place, many)
            clear(main.at[:, planes], left.at[planes], right.at[planes])
            clear(yrecv.at[0, :, planes], yrecv.at[1, :, planes])
            planes = pl.ds(pplace, PITERS)
            clear(scale_all.at[:, planes], coupled_all.at[:, planes])

    x_at = lax.broadcasted_iota(jnp.int32, (2 * nx, 2 * px), 0)
    x_at = jnp.where(x_at < nx + nx // 2, x_at, x_at - 2 * nx)
    column = lax.broadcasted_iota(jnp.int32, (2 * nx, 2 * px), 1)
    offset = x_at - 2 * jnp.where(column < px, column, column - px)
    apart = jnp.where(offset < 0, -offset, offset)
    to_pressure[0] = jnp.where(apart == 0, 0.5, jnp.where(apart == 1, 0.25, 0.0))
    slope = jnp.where(apart == 1, 0.25, jnp.where(apart == 2, 0.125, 0.0))
    to_pressure[1] = jnp.where(offset < 0, -slope, slope)

    for load in loads:
        load.wait()

    lane = lax.broadcasted_iota(jnp.int32, (ny, nx), 1)

    low_rows = lax.broadcasted_iota(jnp.int32, (ROWS, nx), 0) < ROWS // 2

    @pl.loop(0, nz)
    def _(k):
        own = [main[f, BELOW + k] for f in range(FIELDS)]
        edge = own[0]
        for f in range(1, FIELDS):
            moved = pltpu.roll(own[f], GROUP * f, 1)
            inside = jnp.logical_and(lane >= GROUP * f - BELOW, lane < GROUP * f + BELOW)
            edge = jnp.where(inside, moved, edge)
        packed[k] = edge
        for t in range(3):
            low, high = own[2 * t][:ROWS], own[2 * t][-ROWS:]
            if 2 * t + 1 < FIELDS:
                other = own[2 * t + 1]
                low = jnp.where(low_rows, low, pltpu.roll(other[:ROWS], ROWS // 2, 0))
                high = jnp.where(low_rows, pltpu.roll(other[-ROWS:], ROWS // 2, 0), high)
            ysend[0, t, k] = low
            ysend[1, t, k] = high

    scale_own = pscale_in[...]
    scale_all[1, pl.ds(PITERS, pz), pl.ds(0, py), :] = jnp.concatenate([scale_own, scale_own], axis=2)

    pl.semaphore_wait(barrier, count - 1)

    def velocity_copies(d):
        dx, dy, dz = d
        y_from, y_to, y_many = {
            0: (0, 0, ny), 1: (ny - ROWS, ny + ROWS, ROWS), -1: (0, ny, ROWS)}[dy]
        pieces = [(0, 0)] if dx or not dz else [(0, 0), (1, 1)]
        copies = []
        for group, cut in pieces:
            z_from, z_to, z_many = {
                0: (0, BELOW, nz), 1: (nz - BELOW + cut, cut, BELOW - cut),
                -1: (0, BELOW + nz, ABOVE - cut)}[dz]
            if dx:
                source = packed.at[pl.ds(z_from, z_many), pl.ds(y_from, y_many), :]
                place = (left if dx == 1 else right).at[pl.ds(z_to, z_many), pl.ds(y_to, y_many), :]
            elif dy:
                side = 1 if dy == 1 else 0
                tiles = pl.ds(0, 3) if not dz else pl.ds(1, 2) if group else pl.ds(0, 1)
                source = ysend.at[side, tiles, pl.ds(z_from, z_many)]
                place = yrecv.at[side, tiles, pl.ds(z_to, z_many)]
            else:
                fields = pl.ds(DEEP, FIELDS - DEEP) if group else pl.ds(0, DEEP)
                source = main.at[fields, pl.ds(BELOW + z_from, z_many)]
                place = main.at[fields, pl.ds(z_to, z_many)]
            at_sem = DIRECTIONS.index(d)
            which = 3 if group else 0
            copies.append(pltpu.make_async_remote_copy(
                src_ref=source, dst_ref=place, send_sem=send_sem.at[which, at_sem],
                recv_sem=recv_sem.at[which, at_sem], device_id=target(d), device_id_type=MESH))
        return copies

    def pressure_copy(buffer, which, d):
        dx, dy, dz = d
        z_from, z_to, z_many = {
            0: (PITERS, PITERS, pz), 1: (pz, 0, PITERS), -1: (PITERS, PITERS + pz, PITERS)}[dz]
        y_to = {0: 0, 1: 2 * ROWS, -1: ROWS}[dy]
        at_sem = DIRECTIONS.index(d)
        return pltpu.make_async_remote_copy(
            src_ref=buffer.at[1, pl.ds(z_from, z_many), pl.ds(0, ROWS), :],
            dst_ref=buffer.at[1 - dx, pl.ds(z_to, z_many), pl.ds(y_to, ROWS), :],
            send_sem=send_sem.at[which, at_sem], recv_sem=recv_sem.at[which, at_sem],
            device_id=target(d), device_id_type=MESH)

    def opposite(d):
        return tuple(-c for c in d)

    for d in DIRECTIONS:
        @pl.when(exists(d))
        def _(d=d):
            for copy in velocity_copies(d):
                copy.start()

    for d in DIRECTIONS:
        @pl.when(exists(d))
        def _(d=d):
            pressure_copy(scale_all, 1, d).start()

    start_v, steps_v = chebyshev_scalars(vbounds, SWEEPS)
    start_p, steps_p = chebyshev_scalars(pbounds, PITERS)

    def arrive(directions):
        for d in directions:
            @pl.when(exists(opposite(d)))
            def _(d=d):
                for copy in velocity_copies(d):
                    copy.wait_recv()

    arrive([d for d in DIRECTIONS if not d[2]])

    row8 = lax.broadcasted_iota(jnp.int32, (ROWS, nx), 0) < ROWS // 2
    wide_lane = lax.broadcasted_iota(jnp.int32, (ny + ROWS, nx), 1)
    from_right = lax.rem(wide_lane, GROUP) < GROUP // 2

    def fold_rows(block):
        low, up, down = block[:-2 * ROWS], block[-2 * ROWS:-ROWS], block[-ROWS:]
        return jnp.concatenate([low, jnp.where(row8[:, :block.shape[1]], up, down)], axis=0)

    def start_plane(k):
        halo = jnp.where(from_right, fold_rows(right[k]), fold_rows(left[k]))

        def whole(f):
            side = pltpu.roll(halo, nx - GROUP * f, 1) if f else halo
            up, down = yrecv[0, f // 2, k], yrecv[1, f // 2, k]
            if f % 2:
                tile = pltpu.roll(jnp.where(row8, down, up), ROWS // 2, 0)
            else:
                tile = jnp.where(row8, up, down)
            return jnp.concatenate([jnp.concatenate([main[f, k], tile], axis=0), side], axis=1)

        weight = whole(VISCOSITY)
        wide_v[k] = weight
        wide_m[k] = whole(MASS)
        for c in range(3):
            source = whole(COMPONENT[c])
            wide_b[c, k] = source
            smooth[c, k] = average(average(weight * (source * start_v), 1, 0.5, 1.0), 0, 0.5, 1.0)

    def apply_wide(c, k, held, direction, weight):
        mean = held[c, k] + 0.5 * (held[c, k - 1] + held[c, k + 1])
        return weight * (16.0 * (weight * direction) - 2.0 * mean) + wide_m[k] * direction

    def first_sweep(k):
        weight = wide_v[k]
        for c in range(3):
            source = wide_b[c, k]
            first = source * start_v
            rest = source - apply_wide(c, k, smooth, first, weight)
            second = steps_v[0][0] * first + steps_v[0][1] * rest
            resid[c, k] = rest
            direct[c, k] = second
            total[c, k] = first + second
            smooth_next[c, k] = average(average(weight * second, 1, 0.5, 1.0), 0, 0.5, 1.0)

    def second_sweep(k):
        weight = wide_v[k]
        for c in range(3):
            second = direct[c, k]
            rest = resid[c, k] - apply_wide(c, k, smooth_next, second, weight)
            total[c, k] = total[c, k] + (steps_v[1][0] * second + steps_v[1][1] * rest)

    stages = (start_plane, first_sweep, second_sweep)
    for n, stage in enumerate(stages):
        pl.loop(BELOW + n, BELOW + nz - n)(stage)

    arrive([d for d in DIRECTIONS if d[2]])

    for n, stage in enumerate(stages):
        @pl.loop(0, BELOW + ABOVE)
        def _(i, n=n, stage=stage):
            stage(i + jnp.where(i < BELOW, n, nz - n))

    for c in range(3):
        vres[c] = total[c, mid, pl.ds(0, ny), pl.ds(0, nx)]
    store_velocity = pltpu.make_async_copy(vres, vout, local_sem.at[5])
    store_velocity.start()

    for k in range(pz):
        z = BELOW + 2 * k
        for c in range(2):
            gathered[c, k] = 0.5 * total[c, z] + 0.25 * (total[c, z - 1] + total[c, z + 1])
        gathered[2, k] = 0.25 * (total[2, z + 1] - total[2, z - 1]) + 0.125 * (
            total[2, z + 2] - total[2, z - 2])
    wide_rows = ny + ROWS

    def along_x(c, matrix):
        return jnp.dot(
            gathered[c].reshape(pz * wide_rows, 2 * nx), to_pressure[matrix],
            precision=lax.Precision.HIGHEST, preferred_element_type=jnp.float32,
        ).reshape(pz, wide_rows, 2 * px)

    part0, part1, part2 = along_x(0, 1), along_x(1, 0), along_x(2, 0)
    for k in range(pz):
        u = part1[k]
        one = pltpu.roll(u, wide_rows - 1, 0) - pltpu.roll(u, 1, 0)
        two = pltpu.roll(u, wide_rows - 2, 0) - pltpu.roll(u, 2, 0)
        rows_at[k] = average(part0[k] + part2[k], 0, 0.25, 0.5) + (0.25 * one + 0.125 * two)
    for k in range(pz):
        source = prhs_in[k]
        coupled_all[1, PITERS + k, pl.ds(0, py), :] = (
            jnp.concatenate([source, source], axis=1) - rows_at[k, pl.ds(0, py, stride=2), :])

    for d in DIRECTIONS:
        @pl.when(exists(d))
        def _(d=d):
            pressure_copy(coupled_all, 2, d).start()

    for d in DIRECTIONS:
        @pl.when(exists(d))
        def _(d=d):
            for copy in velocity_copies(d):
                copy.wait_send()
            pressure_copy(scale_all, 1, d).wait_send()

    for d in DIRECTIONS:
        @pl.when(exists(opposite(d)))
        def _(d=d):
            pressure_copy(scale_all, 1, d).wait_recv()
            pressure_copy(coupled_all, 2, d).wait_recv()

    narrow_lane = lax.broadcasted_iota(jnp.int32, (py + ROWS, 2 * px), 1)
    deep = pz + 2 * PITERS

    def whole_pressure(buffer, k):
        outside = jnp.where(
            narrow_lane < px + px // 2, fold_rows(buffer[2, k]), fold_rows(buffer[0, k]))
        return jnp.where(narrow_lane < px, fold_rows(buffer[1, k]), outside)

    scales = [whole_pressure(scale_all, k) for k in range(deep)]
    rest = [whole_pressure(coupled_all, k) for k in range(deep)]
    way = [value * start_p for value in rest]
    answer = list(way)
    for n in range(PITERS):
        mean = [
            average(average(scales[k] * way[k], 1, 1 / 6, 2 / 3), 0, 1 / 6, 2 / 3) if n <= k < deep - n else None
            for k in range(deep)]
        for k in range(n + 1, deep - n - 1):
            applied = scales[k] * ((2 / 3) * mean[k] + (1 / 6) * (mean[k - 1] + mean[k + 1]))
            rest[k] = rest[k] - applied
            way[k] = steps_p[n][0] * way[k] + steps_p[n][1] * rest[k]
            answer[k] = answer[k] + way[k]
    for k in range(pz):
        pres[k] = answer[PITERS + k][:py, :px]
    store_pressure = pltpu.make_async_copy(pres, pout, local_sem.at[6])
    store_pressure.start()

    for d in DIRECTIONS:
        @pl.when(exists(d))
        def _(d=d):
            pressure_copy(coupled_all, 2, d).wait_send()
    store_velocity.wait()
    store_pressure.wait()


def per_device(vrhs, prhs, visc, mass, pscale, vbounds, pbounds):
    nz, ny, nx = visc.shape
    pz, py, px = pscale.shape
    depth = BELOW + nz + ABOVE
    wide = (depth, ny + ROWS, 2 * nx)
    f32 = jnp.float32
    anywhere = pl.BlockSpec(memory_space=pl.ANY)
    scalars = pl.BlockSpec(memory_space=pltpu.SMEM)
    ways = len(DIRECTIONS)
    edge = (depth, ny + 2 * ROWS, nx)
    pressure_all = (3, pz + 2 * PITERS, py + 2 * ROWS, 2 * px)
    return pl.pallas_call(
        kernel,
        out_shape=(jax.ShapeDtypeStruct(vrhs.shape, f32), jax.ShapeDtypeStruct(prhs.shape, f32)),
        in_specs=[anywhere] * 5 + [scalars] * 2,
        out_specs=(anywhere, anywhere),
        scratch_shapes=[
            pltpu.VMEM((FIELDS, depth, ny, nx), f32),
            pltpu.VMEM(edge, f32),
            pltpu.VMEM(edge, f32),
            pltpu.VMEM((nz, ny, nx), f32),
            pltpu.VMEM((2, 3, nz, ROWS, nx), f32),
            pltpu.VMEM((2, 3, depth, ROWS, nx), f32),
            pltpu.VMEM((3,) + wide, f32),
            pltpu.VMEM(wide, f32),
            pltpu.VMEM(wide, f32),
            pltpu.VMEM((3,) + wide, f32),
            pltpu.VMEM((3,) + wide, f32),
            pltpu.VMEM((3,) + wide, f32),
            pltpu.VMEM((3,) + wide, f32),
            pltpu.VMEM((3,) + wide, f32),
            pltpu.VMEM((3, pz, ny + ROWS, 2 * nx), f32),
            pltpu.VMEM((pz, py, px), f32),
            pltpu.VMEM((pz, py, px), f32),
            pltpu.VMEM(pressure_all, f32),
            pltpu.VMEM(pressure_all, f32),
            pltpu.VMEM((2, 2 * nx, 2 * px), f32),
            pltpu.VMEM((pz, ny + ROWS, 2 * px), f32),
            pltpu.VMEM((3, nz, ny, nx), f32),
            pltpu.VMEM((pz, py, px), f32),
            pltpu.SemaphoreType.DMA((8,)),
            pltpu.SemaphoreType.DMA((4, ways)),
            pltpu.SemaphoreType.DMA((4, ways)),
        ],
        compiler_params=pltpu.CompilerParams(collective_id=0, has_side_effects=True),
    )(vrhs, prhs, visc, mass, pscale, vbounds, pbounds)


def solution(mesh):
    cells = P("gz", "gy", "gx")
    in_specs = (P(None, "gz", "gy", "gx"), cells, cells, cells, cells, P(), P())
    out_specs = (P(None, "gz", "gy", "gx"), cells)
    return jax.shard_map(
        per_device, mesh=mesh, in_specs=in_specs, out_specs=out_specs, check_vma=False
    )
```

```python
import itertools

import jax
import jax.numpy as jnp
from jax import lax
from jax.experimental import pallas as pl
from jax.experimental.pallas import tpu as pltpu
from jax.sharding import PartitionSpec as P

SWEEPS = 2
PITERS = 2
BELOW = SWEEPS + 2
ABOVE = SWEEPS + 1
ROWS = 8
FIELDS = 5
VISCOSITY, MASS, COMPONENT = 1, 4, (2, 3, 0)
DEEP = 2
SPAN = 32
MESH = pl.DeviceIdType.MESH
AXES = ("gx", "gy", "gz")
DIRECTIONS = [d for d in itertools.product((0, -1, 1), repeat=3) if d != (0, 0, 0)]
DIRECTIONS.sort(key=lambda d: -sum(abs(c) for c in d))
PLANE_FIRST = sorted(DIRECTIONS, key=lambda d: abs(d[2]))


def chebyshev_scalars(bounds, count):
    low, high = bounds[0], bounds[1]
    theta = (high + low) * 0.5
    delta = (high - low) * 0.5
    sigma = theta / delta
    rho = 1.0 / sigma
    steps = []
    for _ in range(count):
        rho_next = 1.0 / (2.0 * sigma - rho)
        steps.append((rho_next * rho, 2.0 * rho_next / delta))
        rho = rho_next
    return 1.0 / theta, steps


def average(value, axis, outer, centre):
    size = value.shape[axis]
    return centre * value + outer * (pltpu.roll(value, 1, axis) + pltpu.roll(value, size - 1, axis))


def kernel(
    vrhs, prhs, visc, mass, pscale, vbounds, pbounds,
    vout, pout,
    main, left, right, packed, ysend, yrecv,
    wide_b, wide_v, wide_m, smooth, smooth_next, resid, direct, total,
    gathered, prhs_in, pscale_in, scale_all, coupled_all, edge_send, edge_recv, to_pressure, rows_at, vres, pres,
    local_sem, send_sem, recv_sem,
):
    nz, ny, nx = visc.shape
    pz, py, px = pscale.shape
    depth = BELOW + nz + ABOVE
    sizes = [lax.axis_size(a) for a in AXES]
    at = [lax.axis_index(a) for a in AXES]

    def exists(d):
        ok = None
        for coordinate, place, size in zip(d, at, sizes):
            if coordinate:
                here = place > 0 if coordinate < 0 else place < size - 1
                ok = here if ok is None else jnp.logical_and(ok, here)
        return ok

    def target(d):
        return {a: p + c for a, p, c in zip(AXES, at, d)}

    mid = pl.ds(BELOW, nz)
    loads = [
        pltpu.make_async_copy(vrhs.at[pl.ds(0, 2)], main.at[pl.ds(2, 2), mid], local_sem.at[0]),
        pltpu.make_async_copy(vrhs.at[2], main.at[0, mid], local_sem.at[7]),
        pltpu.make_async_copy(visc, main.at[VISCOSITY, mid], local_sem.at[1]),
        pltpu.make_async_copy(mass, main.at[MASS, mid], local_sem.at[2]),
        pltpu.make_async_copy(pscale, pscale_in, local_sem.at[3]),
        pltpu.make_async_copy(prhs, prhs_in, local_sem.at[4]),
    ]
    for load in loads:
        load.start()

    barrier = pltpu.get_barrier_semaphore()
    count = None
    for place, size in zip(at, sizes):
        span = 1 + jnp.where(place > 0, 1, 0) + jnp.where(place < size - 1, 1, 0)
        count = span if count is None else count * span
    for d in DIRECTIONS:
        @pl.when(exists(d))
        def _(d=d):
            pl.semaphore_signal(barrier, inc=1, device_id=target(d), device_id_type=MESH)

    def clear(*refs):
        for ref in refs:
            ref[...] = jnp.zeros(ref.shape, jnp.float32)

    for plane in (0, depth - 1):
        for f in range(DEEP, FIELDS):
            clear(main.at[f, plane])
        for side in range(2):
            for t in range(1, 3):
                clear(yrecv.at[side, t, plane])

    def missing(axis, sign):
        return at[axis] == (0 if sign < 0 else sizes[axis] - 1)

    for sign, buffer, slot in ((-1, left, 0), (1, right, 1)):
        @pl.when(missing(0, sign))
        def _(buffer=buffer, slot=slot):
            clear(buffer, edge_recv.at[:, slot])

    for sign, side in ((1, 0), (-1, 1)):
        @pl.when(missing(1, sign))
        def _(side=side):
            rows = pl.ds(ny + side * ROWS, ROWS)
            clear(yrecv.at[side], left.at[:, rows], right.at[:, rows])
            rows = pl.ds(py + side * ROWS, ROWS)
            clear(scale_all.at[:, rows], coupled_all.at[:, rows], edge_recv.at[:, :, :, rows])

    for sign, place, many, pplace in ((-1, 0, BELOW, 0), (1, BELOW + nz, ABOVE, PITERS + pz)):
        @pl.when(missing(2, sign))
        def _(sign=sign, place=place, many=many, pplace=pplace):
            planes = pl.ds(place, many)
            clear(main.at[:, planes], left.at[place // BELOW], right.at[place // BELOW])
            clear(edge_recv.at[:, :, 1 + sign])
            clear(yrecv.at[0, :, planes], yrecv.at[1, :, planes])
            planes = pl.ds(pplace, PITERS)
            clear(scale_all.at[planes], coupled_all.at[planes])

    x_at = lax.broadcasted_iota(jnp.int32, (2 * nx, 2 * px), 0)
    x_at = jnp.where(x_at < nx + nx // 2, x_at, x_at - 2 * nx)
    column = lax.broadcasted_iota(jnp.int32, (2 * nx, 2 * px), 1)
    offset = x_at - 2 * jnp.where(column < px, column, column - px)
    apart = jnp.where(offset < 0, -offset, offset)
    to_pressure[0] = jnp.where(apart == 0, 0.5, jnp.where(apart == 1, 0.25, 0.0))
    slope = jnp.where(apart == 1, 0.25, jnp.where(apart == 2, 0.125, 0.0))
    to_pressure[1] = jnp.where(offset < 0, -slope, slope)

    for load in loads:
        load.wait()

    low_rows = lax.broadcasted_iota(jnp.int32, (ROWS, nx), 0) < ROWS // 2

    @pl.loop(0, nz)
    def _(k):
        own = [main[f, BELOW + k] for f in range(FIELDS)]
        for t in range(3):
            low, high = own[2 * t][:ROWS], own[2 * t][-ROWS:]
            if 2 * t + 1 < FIELDS:
                other = own[2 * t + 1]
                low = jnp.where(low_rows, low, pltpu.roll(other[:ROWS], ROWS // 2, 0))
                high = jnp.where(low_rows, pltpu.roll(other[-ROWS:], ROWS // 2, 0), high)
            ysend[0, t, k] = low
            ysend[1, t, k] = high

    lane = lax.broadcasted_iota(jnp.int32, (ny, nx), 1)

    @pl.loop(0, nz // BELOW)
    def _(g):
        edges = [jnp.zeros((ny, nx), jnp.float32)] * 2
        for z in range(BELOW):
            for f in range(FIELDS):
                value = main[f, BELOW + BELOW * g + z]
                at_lane = SPAN * z + BELOW * f
                inside = jnp.logical_and(lane >= at_lane, lane < at_lane + BELOW)
                for side in range(2):
                    moved = pltpu.roll(value, at_lane + BELOW * side, 1) if at_lane + side else value
                    edges[side] = jnp.where(inside, moved, edges[side])
        for side in range(2):
            packed[side, g] = edges[side]

    def pack_pressure(which, planes):
        edge = planes[0]
        place = lax.broadcasted_iota(jnp.int32, (py, 2 * px), 1)
        for z, value in enumerate(planes):
            for side in range(2):
                at_lane = 4 * z + 2 * side
                inside = jnp.logical_and(place >= at_lane, place < at_lane + 2)
                moved = pltpu.roll(value, 4 * (z + side), 1) if z + side else value
                edge = jnp.where(inside, moved, edge)
        edge_send[which] = edge

    scale_own = [jnp.concatenate([pscale_in[k], pscale_in[k]], axis=1) for k in range(pz)]
    for k in range(pz):
        scale_all[PITERS + k, pl.ds(0, py), :] = scale_own[k]
    pack_pressure(0, scale_own)

    pl.semaphore_wait(barrier, count - 1)

    def velocity_copies(d):
        dx, dy, dz = d
        y_from, y_to, y_many = {
            0: (0, 0, ny), 1: (ny - ROWS, ny + ROWS, ROWS), -1: (0, ny, ROWS)}[dy]
        pieces = [(0, 0)] if dx or not dz else [(0, 0), (1, 1)]
        copies = []
        for group, cut in pieces:
            z_from, z_to, z_many = {
                0: (0, BELOW, nz), 1: (nz - BELOW + cut, cut, BELOW - cut),
                -1: (0, BELOW + nz, ABOVE - cut)}[dz]
            if dx:
                groups = nz // BELOW
                g_from, g_to, g_many = {
                    0: (0, 1, groups), 1: (groups - 1, 0, 1), -1: (0, groups + 1, 1)}[dz]
                side = 1 if dx == 1 else 0
                source = packed.at[side, pl.ds(g_from, g_many), pl.ds(y_from, y_many), :]
                place = (left if side else right).at[pl.ds(g_to, g_many), pl.ds(y_to, y_many), :]
            elif dy:
                side = 1 if dy == 1 else 0
                tiles = pl.ds(0, 3) if not dz else pl.ds(1, 2) if group else pl.ds(0, 1)
                source = ysend.at[side, tiles, pl.ds(z_from, z_many)]
                place = yrecv.at[side, tiles, pl.ds(z_to, z_many)]
            else:
                fields = pl.ds(DEEP, FIELDS - DEEP) if group else pl.ds(0, DEEP)
                source = main.at[fields, pl.ds(BELOW + z_from, z_many)]
                place = main.at[fields, pl.ds(z_to, z_many)]
            at_sem = DIRECTIONS.index(d)
            which = 3 if group else 0
            copies.append(pltpu.make_async_remote_copy(
                src_ref=source, dst_ref=place, send_sem=send_sem.at[which, at_sem],
                recv_sem=recv_sem.at[which, at_sem], device_id=target(d), device_id_type=MESH))
        return copies

    def pressure_copy(buffer, which, d):
        dx, dy, dz = d
        z_from, z_to, z_many = {
            0: (PITERS, PITERS, pz), 1: (pz, 0, PITERS), -1: (PITERS, PITERS + pz, PITERS)}[dz]
        y_to = {0: 0, 1: 2 * ROWS, -1: ROWS}[dy]
        at_sem = DIRECTIONS.index(d)
        if dx:
            source = edge_send.at[which - 1]
            place = edge_recv.at[which - 1, (1 - dx) // 2, 1 - dz, pl.ds(y_to, ROWS)]
        else:
            source = buffer.at[pl.ds(z_from, z_many), pl.ds(0, ROWS), :]
            place = buffer.at[pl.ds(z_to, z_many), pl.ds(y_to, ROWS), :]
        return pltpu.make_async_remote_copy(
            src_ref=source, dst_ref=place,
            send_sem=send_sem.at[which, at_sem], recv_sem=recv_sem.at[which, at_sem],
            device_id=target(d), device_id_type=MESH)

    def opposite(d):
        return tuple(-c for c in d)

    for d in PLANE_FIRST:
        @pl.when(exists(d))
        def _(d=d):
            for copy in velocity_copies(d):
                copy.start()

    for d in DIRECTIONS:
        @pl.when(exists(d))
        def _(d=d):
            pressure_copy(scale_all, 1, d).start()

    start_v, steps_v = chebyshev_scalars(vbounds, SWEEPS)
    start_p, steps_p = chebyshev_scalars(pbounds, PITERS)

    def arrive(directions):
        for d in directions:
            @pl.when(exists(opposite(d)))
            def _(d=d):
                for copy in velocity_copies(d):
                    copy.wait_recv()

    arrive([d for d in DIRECTIONS if not d[2]])

    row8 = lax.broadcasted_iota(jnp.int32, (ROWS, nx), 0) < ROWS // 2
    wide_lane = lax.broadcasted_iota(jnp.int32, (ny + ROWS, nx), 1)
    from_right = wide_lane < nx // 2

    def fold_rows(block):
        low, up, down = block[:-2 * ROWS], block[-2 * ROWS:-ROWS], block[-ROWS:]
        return jnp.concatenate([low, jnp.where(row8[:, :block.shape[1]], up, down)], axis=0)

    def start_plane(k):
        group = lax.div(k, BELOW)
        shift = SPAN * (k - BELOW * group)
        near = pltpu.roll(fold_rows(right[group]), lax.rem(nx - shift, nx), 1)
        far = pltpu.roll(fold_rows(left[group]), nx - BELOW - shift, 1)

        def whole(f):
            side = jnp.where(from_right, near, far) if not f else jnp.where(
                from_right, pltpu.roll(near, nx - BELOW * f, 1), pltpu.roll(far, nx - BELOW * f, 1))
            up, down = yrecv[0, f // 2, k], yrecv[1, f // 2, k]
            if f % 2:
                tile = pltpu.roll(jnp.where(row8, down, up), ROWS // 2, 0)
            else:
                tile = jnp.where(row8, up, down)
            return jnp.concatenate([jnp.concatenate([main[f, k], tile], axis=0), side], axis=1)

        weight = whole(VISCOSITY)
        wide_v[k] = weight
        wide_m[k] = whole(MASS)
        for c in range(3):
            source = whole(COMPONENT[c])
            wide_b[c, k] = source
            smooth[c, k] = average(average(weight * (source * start_v), 1, 0.5, 1.0), 0, 0.5, 1.0)

    def apply_wide(c, k, held, direction, weight):
        mean = held[c, k] + 0.5 * (held[c, k - 1] + held[c, k + 1])
        return weight * (16.0 * (weight * direction) - 2.0 * mean) + wide_m[k] * direction

    def first_sweep(k):
        weight = wide_v[k]
        for c in range(3):
            source = wide_b[c, k]
            first = source * start_v
            rest = source - apply_wide(c, k, smooth, first, weight)
            second = steps_v[0][0] * first + steps_v[0][1] * rest
            resid[c, k] = rest
            direct[c, k] = second
            total[c, k] = first + second
            smooth_next[c, k] = average(average(weight * second, 1, 0.5, 1.0), 0, 0.5, 1.0)

    def second_sweep(k):
        weight = wide_v[k]
        for c in range(3):
            second = direct[c, k]
            rest = resid[c, k] - apply_wide(c, k, smooth_next, second, weight)
            total[c, k] = total[c, k] + (steps_v[1][0] * second + steps_v[1][1] * rest)

    stages = (start_plane, first_sweep, second_sweep)
    for n, stage in enumerate(stages):
        pl.loop(BELOW + n, BELOW + nz - n)(stage)

    arrive([d for d in DIRECTIONS if d[2]])

    for n, stage in enumerate(stages):
        @pl.loop(0, BELOW + ABOVE)
        def _(i, n=n, stage=stage):
            stage(i + jnp.where(i < BELOW, n, nz - n))

    for c in range(3):
        vres[c] = total[c, mid, pl.ds(0, ny), pl.ds(0, nx)]
    store_velocity = pltpu.make_async_copy(vres, vout, local_sem.at[5])
    store_velocity.start()

    for k in range(pz):
        z = BELOW + 2 * k
        for c in range(2):
            gathered[c, k] = 0.5 * total[c, z] + 0.25 * (total[c, z - 1] + total[c, z + 1])
        gathered[2, k] = 0.25 * (total[2, z + 1] - total[2, z - 1]) + 0.125 * (
            total[2, z + 2] - total[2, z - 2])
    wide_rows = ny + ROWS

    def along_x(c, matrix):
        return jnp.dot(
            gathered[c].reshape(pz * wide_rows, 2 * nx), to_pressure[matrix],
            precision=lax.Precision.HIGHEST, preferred_element_type=jnp.float32,
        ).reshape(pz, wide_rows, 2 * px)

    part0, part1, part2 = along_x(0, 1), along_x(1, 0), along_x(2, 0)
    for k in range(pz):
        u = part1[k]
        one = pltpu.roll(u, wide_rows - 1, 0) - pltpu.roll(u, 1, 0)
        two = pltpu.roll(u, wide_rows - 2, 0) - pltpu.roll(u, 2, 0)
        rows_at[k] = average(part0[k] + part2[k], 0, 0.25, 0.5) + (0.25 * one + 0.125 * two)
    coupled_own = []
    for k in range(pz):
        source = prhs_in[k]
        coupled_own.append(
            jnp.concatenate([source, source], axis=1) - rows_at[k, pl.ds(0, py, stride=2), :])
        coupled_all[PITERS + k, pl.ds(0, py), :] = coupled_own[k]
    pack_pressure(1, coupled_own)

    for d in DIRECTIONS:
        @pl.when(exists(d))
        def _(d=d):
            pressure_copy(coupled_all, 2, d).start()

    for d in DIRECTIONS:
        @pl.when(exists(d))
        def _(d=d):
            for copy in velocity_copies(d):
                copy.wait_send()
            pressure_copy(scale_all, 1, d).wait_send()

    for d in DIRECTIONS:
        @pl.when(exists(opposite(d)))
        def _(d=d):
            pressure_copy(scale_all, 1, d).wait_recv()
            pressure_copy(coupled_all, 2, d).wait_recv()

    narrow_lane = lax.broadcasted_iota(jnp.int32, (py + ROWS, 2 * px), 1)
    deep = pz + 2 * PITERS

    def whole_pressure(buffer, which, k):
        slot, z = (0, pz - PITERS + k) if k < PITERS else (
            (1, k - PITERS) if k < PITERS + pz else (2, k - PITERS - pz))
        near = pltpu.roll(fold_rows(edge_recv[which, 1, slot]), px - 4 * z, 1)
        far = pltpu.roll(fold_rows(edge_recv[which, 0, slot]), 2 * px - 4 - 4 * z, 1)
        outside = jnp.where(narrow_lane < px + px // 2, near, far)
        return jnp.where(narrow_lane < px, fold_rows(buffer[k]), outside)

    scales = [whole_pressure(scale_all, 0, k) for k in range(deep)]
    rest = [whole_pressure(coupled_all, 1, k) for k in range(deep)]
    way = [value * start_p for value in rest]
    answer = list(way)
    for n in range(PITERS):
        mean = [
            average(average(scales[k] * way[k], 1, 1 / 6, 2 / 3), 0, 1 / 6, 2 / 3) if n <= k < deep - n else None
            for k in range(deep)]
        for k in range(n + 1, deep - n - 1):
            applied = scales[k] * ((2 / 3) * mean[k] + (1 / 6) * (mean[k - 1] + mean[k + 1]))
            rest[k] = rest[k] - applied
            way[k] = steps_p[n][0] * way[k] + steps_p[n][1] * rest[k]
            answer[k] = answer[k] + way[k]
    for k in range(pz):
        pres[k] = answer[PITERS + k][:py, :px]
    store_pressure = pltpu.make_async_copy(pres, pout, local_sem.at[6])
    store_pressure.start()

    for d in DIRECTIONS:
        @pl.when(exists(d))
        def _(d=d):
            pressure_copy(coupled_all, 2, d).wait_send()
    store_velocity.wait()
    store_pressure.wait()


def per_device(vrhs, prhs, visc, mass, pscale, vbounds, pbounds):
    nz, ny, nx = visc.shape
    pz, py, px = pscale.shape
    depth = BELOW + nz + ABOVE
    wide = (depth, ny + ROWS, 2 * nx)
    f32 = jnp.float32
    anywhere = pl.BlockSpec(memory_space=pl.ANY)
    scalars = pl.BlockSpec(memory_space=pltpu.SMEM)
    ways = len(DIRECTIONS)
    edge = (nz // BELOW + 2, ny + 2 * ROWS, nx)
    pressure_all = (pz + 2 * PITERS, py + 2 * ROWS, 2 * px)
    return pl.pallas_call(
        kernel,
        out_shape=(jax.ShapeDtypeStruct(vrhs.shape, f32), jax.ShapeDtypeStruct(prhs.shape, f32)),
        in_specs=[anywhere] * 5 + [scalars] * 2,
        out_specs=(anywhere, anywhere),
        scratch_shapes=[
            pltpu.VMEM((FIELDS, depth, ny, nx), f32),
            pltpu.VMEM(edge, f32),
            pltpu.VMEM(edge, f32),
            pltpu.VMEM((2, nz // BELOW, ny, nx), f32),
            pltpu.VMEM((2, 3, nz, ROWS, nx), f32),
            pltpu.VMEM((2, 3, depth, ROWS, nx), f32),
            pltpu.VMEM((3,) + wide, f32),
            pltpu.VMEM(wide, f32),
            pltpu.VMEM(wide, f32),
            pltpu.VMEM((3,) + wide, f32),
            pltpu.VMEM((3,) + wide, f32),
            pltpu.VMEM((3,) + wide, f32),
            pltpu.VMEM((3,) + wide, f32),
            pltpu.VMEM((3,) + wide, f32),
            pltpu.VMEM((3, pz, ny + ROWS, 2 * nx), f32),
            pltpu.VMEM((pz, py, px), f32),
            pltpu.VMEM((pz, py, px), f32),
            pltpu.VMEM(pressure_all, f32),
            pltpu.VMEM(pressure_all, f32),
            pltpu.VMEM((2, py, 2 * px), f32),
            pltpu.VMEM((2, 2, 3, py + 2 * ROWS, 2 * px), f32),
            pltpu.VMEM((2, 2 * nx, 2 * px), f32),
            pltpu.VMEM((pz, ny + ROWS, 2 * px), f32),
            pltpu.VMEM((3, nz, ny, nx), f32),
            pltpu.VMEM((pz, py, px), f32),
            pltpu.SemaphoreType.DMA((8,)),
            pltpu.SemaphoreType.DMA((4, ways)),
            pltpu.SemaphoreType.DMA((4, ways)),
        ],
        compiler_params=pltpu.CompilerParams(collective_id=0, has_side_effects=True),
    )(vrhs, prhs, visc, mass, pscale, vbounds, pbounds)


def solution(mesh):
    cells = P("gz", "gy", "gx")
    in_specs = (P(None, "gz", "gy", "gx"), cells, cells, cells, cells, P(), P())
    out_specs = (P(None, "gz", "gy", "gx"), cells)
    return jax.shard_map(
        per_device, mesh=mesh, in_specs=in_specs, out_specs=out_specs, check_vma=False
    )
```

```python
import itertools

import jax
import jax.numpy as jnp
from jax import lax
from jax.experimental import pallas as pl
from jax.experimental.pallas import tpu as pltpu
from jax.sharding import PartitionSpec as P

SWEEPS = 2
PITERS = 2
BELOW = SWEEPS + 2
ABOVE = SWEEPS + 1
ROWS = 8
FIELDS = 5
VISCOSITY, MASS, COMPONENT = 1, 4, (2, 3, 0)
DEEP = 2
SPAN = 32
MESH = pl.DeviceIdType.MESH
AXES = ("gx", "gy", "gz")
DIRECTIONS = [d for d in itertools.product((0, -1, 1), repeat=3) if d != (0, 0, 0)]
DIRECTIONS.sort(key=lambda d: -sum(abs(c) for c in d))
PLANE_FIRST = sorted(DIRECTIONS, key=lambda d: abs(d[2]))


def chebyshev_scalars(bounds, count):
    low, high = bounds[0], bounds[1]
    theta = (high + low) * 0.5
    delta = (high - low) * 0.5
    sigma = theta / delta
    rho = 1.0 / sigma
    steps = []
    for _ in range(count):
        rho_next = 1.0 / (2.0 * sigma - rho)
        steps.append((rho_next * rho, 2.0 * rho_next / delta))
        rho = rho_next
    return 1.0 / theta, steps


def average(value, axis, outer, centre):
    size = value.shape[axis]
    return centre * value + outer * (pltpu.roll(value, 1, axis) + pltpu.roll(value, size - 1, axis))


def kernel(
    vrhs, prhs, visc, mass, pscale, vbounds, pbounds,
    vout, pout,
    main, left, right, packed, ysend, yrecv,
    wide_b, wide_v, wide_m, smooth, smooth_next, resid, direct, total,
    gathered, prhs_in, pscale_in, scale_all, coupled_all, edge_send, edge_recv, to_pressure, rows_at, vres, pres,
    local_sem, send_sem, recv_sem,
):
    nz, ny, nx = visc.shape
    pz, py, px = pscale.shape
    depth = BELOW + nz + ABOVE
    sizes = [lax.axis_size(a) for a in AXES]
    at = [lax.axis_index(a) for a in AXES]

    def exists(d):
        ok = None
        for coordinate, place, size in zip(d, at, sizes):
            if coordinate:
                here = place > 0 if coordinate < 0 else place < size - 1
                ok = here if ok is None else jnp.logical_and(ok, here)
        return ok

    def target(d):
        return {a: p + c for a, p, c in zip(AXES, at, d)}

    mid = pl.ds(BELOW, nz)
    loads = [
        pltpu.make_async_copy(vrhs.at[pl.ds(0, 2)], main.at[pl.ds(2, 2), mid], local_sem.at[0]),
        pltpu.make_async_copy(vrhs.at[2], main.at[0, mid], local_sem.at[7]),
        pltpu.make_async_copy(visc, main.at[VISCOSITY, mid], local_sem.at[1]),
        pltpu.make_async_copy(mass, main.at[MASS, mid], local_sem.at[2]),
        pltpu.make_async_copy(pscale, pscale_in, local_sem.at[3]),
        pltpu.make_async_copy(prhs, prhs_in, local_sem.at[4]),
    ]
    for load in loads:
        load.start()

    barrier = pltpu.get_barrier_semaphore()
    count = None
    for place, size in zip(at, sizes):
        span = 1 + jnp.where(place > 0, 1, 0) + jnp.where(place < size - 1, 1, 0)
        count = span if count is None else count * span
    for d in DIRECTIONS:
        @pl.when(exists(d))
        def _(d=d):
            pl.semaphore_signal(barrier, inc=1, device_id=target(d), device_id_type=MESH)

    def clear(*refs):
        for ref in refs:
            ref[...] = jnp.zeros(ref.shape, jnp.float32)

    for plane in (0, depth - 1):
        for f in range(DEEP, FIELDS):
            clear(main.at[f, plane])
        for side in range(2):
            for t in range(1, 3):
                clear(yrecv.at[side, t, plane])

    def missing(axis, sign):
        return at[axis] == (0 if sign < 0 else sizes[axis] - 1)

    for sign, buffer, slot in ((-1, left, 0), (1, right, 1)):
        @pl.when(missing(0, sign))
        def _(buffer=buffer, slot=slot):
            clear(buffer, edge_recv.at[:, slot])

    for sign, side in ((1, 0), (-1, 1)):
        @pl.when(missing(1, sign))
        def _(side=side):
            rows = pl.ds(ny + side * ROWS, ROWS)
            clear(yrecv.at[side], left.at[:, rows], right.at[:, rows])
            rows = pl.ds(py + side * ROWS, ROWS)
            clear(scale_all.at[:, rows], coupled_all.at[:, rows], edge_recv.at[:, :, :, rows])

    for sign, place, many, pplace in ((-1, 0, BELOW, 0), (1, BELOW + nz, ABOVE, PITERS + pz)):
        @pl.when(missing(2, sign))
        def _(sign=sign, place=place, many=many, pplace=pplace):
            planes = pl.ds(place, many)
            clear(main.at[:, planes], left.at[place // BELOW], right.at[place // BELOW])
            clear(edge_recv.at[:, :, 1 + sign])
            clear(yrecv.at[0, :, planes], yrecv.at[1, :, planes])
            planes = pl.ds(pplace, PITERS)
            clear(scale_all.at[planes], coupled_all.at[planes])

    x_at = lax.broadcasted_iota(jnp.int32, (2 * nx, 2 * px), 0)
    x_at = jnp.where(x_at < nx + nx // 2, x_at, x_at - 2 * nx)
    column = lax.broadcasted_iota(jnp.int32, (2 * nx, 2 * px), 1)
    offset = x_at - 2 * jnp.where(column < px, column, column - px)
    apart = jnp.where(offset < 0, -offset, offset)
    to_pressure[0] = jnp.where(apart == 0, 0.5, jnp.where(apart == 1, 0.25, 0.0))
    slope = jnp.where(apart == 1, 0.25, jnp.where(apart == 2, 0.125, 0.0))
    to_pressure[1] = jnp.where(offset < 0, -slope, slope)

    for load in loads:
        load.wait()

    low_rows = lax.broadcasted_iota(jnp.int32, (ROWS, nx), 0) < ROWS // 2

    @pl.loop(0, nz)
    def _(k):
        own = [main[f, BELOW + k] for f in range(FIELDS)]
        for t in range(3):
            low, high = own[2 * t][:ROWS], own[2 * t][-ROWS:]
            if 2 * t + 1 < FIELDS:
                other = own[2 * t + 1]
                low = jnp.where(low_rows, low, pltpu.roll(other[:ROWS], ROWS // 2, 0))
                high = jnp.where(low_rows, pltpu.roll(other[-ROWS:], ROWS // 2, 0), high)
            ysend[0, t, k] = low
            ysend[1, t, k] = high

    lane = lax.broadcasted_iota(jnp.int32, (ny, nx), 1)

    @pl.loop(0, nz // BELOW)
    def _(g):
        edges = [jnp.zeros((ny, nx), jnp.float32)] * 2
        for z in range(BELOW):
            for f in range(FIELDS):
                value = main[f, BELOW + BELOW * g + z]
                at_lane = SPAN * z + BELOW * f
                inside = jnp.logical_and(lane >= at_lane, lane < at_lane + BELOW)
                for side in range(2):
                    moved = pltpu.roll(value, at_lane + BELOW * side, 1) if at_lane + side else value
                    edges[side] = jnp.where(inside, moved, edges[side])
        for side in range(2):
            packed[side, g] = edges[side]

    def pack_pressure(which, planes):
        edge = planes[0]
        place = lax.broadcasted_iota(jnp.int32, (py, 2 * px), 1)
        for z, value in enumerate(planes):
            for side in range(2):
                at_lane = 4 * z + 2 * side
                inside = jnp.logical_and(place >= at_lane, place < at_lane + 2)
                moved = pltpu.roll(value, 4 * (z + side), 1) if z + side else value
                edge = jnp.where(inside, moved, edge)
        edge_send[which] = edge

    scale_own = [jnp.concatenate([pscale_in[k], pscale_in[k]], axis=1) for k in range(pz)]
    for k in range(pz):
        scale_all[PITERS + k, pl.ds(0, py), :] = scale_own[k]
    pack_pressure(0, scale_own)

    pl.semaphore_wait(barrier, count - 1)

    def velocity_copies(d):
        dx, dy, dz = d
        y_from, y_to, y_many = {
            0: (0, 0, ny), 1: (ny - ROWS, ny + ROWS, ROWS), -1: (0, ny, ROWS)}[dy]
        pieces = [(0, 0)] if dx or not dz else [(0, 0), (1, 1)]
        copies = []
        for group, cut in pieces:
            z_from, z_to, z_many = {
                0: (0, BELOW, nz), 1: (nz - BELOW + cut, cut, BELOW - cut),
                -1: (0, BELOW + nz, ABOVE - cut)}[dz]
            if dx:
                groups = nz // BELOW
                g_from, g_to, g_many = {
                    0: (0, 1, groups), 1: (groups - 1, 0, 1), -1: (0, groups + 1, 1)}[dz]
                side = 1 if dx == 1 else 0
                source = packed.at[side, pl.ds(g_from, g_many), pl.ds(y_from, y_many), :]
                place = (left if side else right).at[pl.ds(g_to, g_many), pl.ds(y_to, y_many), :]
            elif dy:
                side = 1 if dy == 1 else 0
                tiles = pl.ds(0, 3) if not dz else pl.ds(1, 2) if group else pl.ds(0, 1)
                source = ysend.at[side, tiles, pl.ds(z_from, z_many)]
                place = yrecv.at[side, tiles, pl.ds(z_to, z_many)]
            else:
                fields = pl.ds(DEEP, FIELDS - DEEP) if group else pl.ds(0, DEEP)
                source = main.at[fields, pl.ds(BELOW + z_from, z_many)]
                place = main.at[fields, pl.ds(z_to, z_many)]
            at_sem = DIRECTIONS.index(d)
            which = 3 if group else 0
            copies.append(pltpu.make_async_remote_copy(
                src_ref=source, dst_ref=place, send_sem=send_sem.at[which, at_sem],
                recv_sem=recv_sem.at[which, at_sem], device_id=target(d), device_id_type=MESH))
        return copies

    def pressure_copy(buffer, which, d):
        dx, dy, dz = d
        z_from, z_to, z_many = {
            0: (PITERS, PITERS, pz), 1: (pz, 0, PITERS), -1: (PITERS, PITERS + pz, PITERS)}[dz]
        y_to = {0: 0, 1: 2 * ROWS, -1: ROWS}[dy]
        at_sem = DIRECTIONS.index(d)
        if dx:
            source = edge_send.at[which - 1]
            place = edge_recv.at[which - 1, (1 - dx) // 2, 1 - dz, pl.ds(y_to, ROWS)]
        else:
            source = buffer.at[pl.ds(z_from, z_many), pl.ds(0, ROWS), :]
            place = buffer.at[pl.ds(z_to, z_many), pl.ds(y_to, ROWS), :]
        return pltpu.make_async_remote_copy(
            src_ref=source, dst_ref=place,
            send_sem=send_sem.at[which, at_sem], recv_sem=recv_sem.at[which, at_sem],
            device_id=target(d), device_id_type=MESH)

    def opposite(d):
        return tuple(-c for c in d)

    for d in PLANE_FIRST:
        @pl.when(exists(d))
        def _(d=d):
            for copy in velocity_copies(d):
                copy.start()

    for d in DIRECTIONS:
        @pl.when(exists(d))
        def _(d=d):
            pressure_copy(scale_all, 1, d).start()

    start_v, steps_v = chebyshev_scalars(vbounds, SWEEPS)
    start_p, steps_p = chebyshev_scalars(pbounds, PITERS)

    def arrive(directions):
        for d in directions:
            @pl.when(exists(opposite(d)))
            def _(d=d):
                for copy in velocity_copies(d):
                    copy.wait_recv()

    arrive([d for d in DIRECTIONS if not d[2]])

    row8 = lax.broadcasted_iota(jnp.int32, (ROWS, nx), 0) < ROWS // 2
    wide_lane = lax.broadcasted_iota(jnp.int32, (ny + ROWS, nx), 1)

    def fold_rows(block):
        low, up, down = block[:-2 * ROWS], block[-2 * ROWS:-ROWS], block[-ROWS:]
        return jnp.concatenate([low, jnp.where(row8[:, :block.shape[1]], up, down)], axis=0)

    def start_plane(k):
        group = k // BELOW
        shift = SPAN * (k - BELOW * group)
        near = fold_rows(right[group])
        near = pltpu.roll(near, nx - shift, 1) if shift else near
        far = pltpu.roll(fold_rows(left[group]), nx - BELOW - shift, 1)

        def whole(f):
            from_right = jnp.logical_and(wide_lane >= BELOW * f, wide_lane < BELOW * f + nx // 2)
            side = jnp.where(from_right, near, far)
            side = pltpu.roll(side, nx - BELOW * f, 1) if f else side
            up, down = yrecv[0, f // 2, k], yrecv[1, f // 2, k]
            if f % 2:
                tile = pltpu.roll(jnp.where(row8, down, up), ROWS // 2, 0)
            else:
                tile = jnp.where(row8, up, down)
            return jnp.concatenate([jnp.concatenate([main[f, k], tile], axis=0), side], axis=1)

        weight = whole(VISCOSITY)
        wide_v[k] = weight
        wide_m[k] = whole(MASS)
        for c in range(3):
            source = whole(COMPONENT[c])
            wide_b[c, k] = source
            smooth[c, k] = average(average(weight * (source * start_v), 1, 0.5, 1.0), 0, 0.5, 1.0)

    def apply_wide(c, k, held, direction, weight):
        mean = held[c, k] + 0.5 * (held[c, k - 1] + held[c, k + 1])
        return weight * (16.0 * (weight * direction) - 2.0 * mean) + wide_m[k] * direction

    def first_sweep(k):
        weight = wide_v[k]
        for c in range(3):
            source = wide_b[c, k]
            first = source * start_v
            rest = source - apply_wide(c, k, smooth, first, weight)
            second = steps_v[0][0] * first + steps_v[0][1] * rest
            resid[c, k] = rest
            direct[c, k] = second
            total[c, k] = first + second
            smooth_next[c, k] = average(average(weight * second, 1, 0.5, 1.0), 0, 0.5, 1.0)

    def second_sweep(k):
        weight = wide_v[k]
        for c in range(3):
            second = direct[c, k]
            rest = resid[c, k] - apply_wide(c, k, smooth_next, second, weight)
            total[c, k] = total[c, k] + (steps_v[1][0] * second + steps_v[1][1] * rest)

    stages = (start_plane, first_sweep, second_sweep)
    for n, stage in enumerate(stages):
        for k in range(BELOW + n, BELOW + nz - n):
            stage(k)

    arrive([d for d in DIRECTIONS if d[2]])

    for n, stage in enumerate(stages):
        for i in range(BELOW + ABOVE):
            stage(i + (n if i < BELOW else nz - n))

    for c in range(3):
        vres[c] = total[c, mid, pl.ds(0, ny), pl.ds(0, nx)]
    store_velocity = pltpu.make_async_copy(vres, vout, local_sem.at[5])
    store_velocity.start()

    for k in range(pz):
        z = BELOW + 2 * k
        for c in range(2):
            gathered[c, k] = 0.5 * total[c, z] + 0.25 * (total[c, z - 1] + total[c, z + 1])
        gathered[2, k] = 0.25 * (total[2, z + 1] - total[2, z - 1]) + 0.125 * (
            total[2, z + 2] - total[2, z - 2])
    wide_rows = ny + ROWS

    def along_x(c, matrix):
        return jnp.dot(
            gathered[c].reshape(pz * wide_rows, 2 * nx), to_pressure[matrix],
            precision=lax.Precision.HIGHEST, preferred_element_type=jnp.float32,
        ).reshape(pz, wide_rows, 2 * px)

    part0, part1, part2 = along_x(0, 1), along_x(1, 0), along_x(2, 0)
    for k in range(pz):
        u = part1[k]
        one = pltpu.roll(u, wide_rows - 1, 0) - pltpu.roll(u, 1, 0)
        two = pltpu.roll(u, wide_rows - 2, 0) - pltpu.roll(u, 2, 0)
        rows_at[k] = average(part0[k] + part2[k], 0, 0.25, 0.5) + (0.25 * one + 0.125 * two)
    coupled_own = []
    for k in range(pz):
        source = prhs_in[k]
        coupled_own.append(
            jnp.concatenate([source, source], axis=1) - rows_at[k, pl.ds(0, py, stride=2), :])
        coupled_all[PITERS + k, pl.ds(0, py), :] = coupled_own[k]
    pack_pressure(1, coupled_own)

    for d in DIRECTIONS:
        @pl.when(exists(d))
        def _(d=d):
            pressure_copy(coupled_all, 2, d).start()

    for d in DIRECTIONS:
        @pl.when(exists(d))
        def _(d=d):
            for copy in velocity_copies(d):
                copy.wait_send()
            pressure_copy(scale_all, 1, d).wait_send()

    for d in DIRECTIONS:
        @pl.when(exists(opposite(d)))
        def _(d=d):
            pressure_copy(scale_all, 1, d).wait_recv()
            pressure_copy(coupled_all, 2, d).wait_recv()

    narrow_lane = lax.broadcasted_iota(jnp.int32, (py + ROWS, 2 * px), 1)
    deep = pz + 2 * PITERS

    def whole_pressure(buffer, which, k):
        slot, z = (0, pz - PITERS + k) if k < PITERS else (
            (1, k - PITERS) if k < PITERS + pz else (2, k - PITERS - pz))
        near = pltpu.roll(fold_rows(edge_recv[which, 1, slot]), px - 4 * z, 1)
        far = pltpu.roll(fold_rows(edge_recv[which, 0, slot]), 2 * px - 4 - 4 * z, 1)
        outside = jnp.where(narrow_lane < px + px // 2, near, far)
        return jnp.where(narrow_lane < px, fold_rows(buffer[k]), outside)

    scales = [whole_pressure(scale_all, 0, k) for k in range(deep)]
    rest = [whole_pressure(coupled_all, 1, k) for k in range(deep)]
    way = [value * start_p for value in rest]
    answer = list(way)
    for n in range(PITERS):
        mean = [
            average(average(scales[k] * way[k], 1, 1 / 6, 2 / 3), 0, 1 / 6, 2 / 3) if n <= k < deep - n else None
            for k in range(deep)]
        for k in range(n + 1, deep - n - 1):
            applied = scales[k] * ((2 / 3) * mean[k] + (1 / 6) * (mean[k - 1] + mean[k + 1]))
            rest[k] = rest[k] - applied
            way[k] = steps_p[n][0] * way[k] + steps_p[n][1] * rest[k]
            answer[k] = answer[k] + way[k]
    for k in range(pz):
        pres[k] = answer[PITERS + k][:py, :px]
    store_pressure = pltpu.make_async_copy(pres, pout, local_sem.at[6])
    store_pressure.start()

    for d in DIRECTIONS:
        @pl.when(exists(d))
        def _(d=d):
            pressure_copy(coupled_all, 2, d).wait_send()
    store_velocity.wait()
    store_pressure.wait()


def per_device(vrhs, prhs, visc, mass, pscale, vbounds, pbounds):
    nz, ny, nx = visc.shape
    pz, py, px = pscale.shape
    depth = BELOW + nz + ABOVE
    wide = (depth, ny + ROWS, 2 * nx)
    f32 = jnp.float32
    anywhere = pl.BlockSpec(memory_space=pl.ANY)
    scalars = pl.BlockSpec(memory_space=pltpu.SMEM)
    ways = len(DIRECTIONS)
    edge = (nz // BELOW + 2, ny + 2 * ROWS, nx)
    pressure_all = (pz + 2 * PITERS, py + 2 * ROWS, 2 * px)
    return pl.pallas_call(
        kernel,
        out_shape=(jax.ShapeDtypeStruct(vrhs.shape, f32), jax.ShapeDtypeStruct(prhs.shape, f32)),
        in_specs=[anywhere] * 5 + [scalars] * 2,
        out_specs=(anywhere, anywhere),
        scratch_shapes=[
            pltpu.VMEM((FIELDS, depth, ny, nx), f32),
            pltpu.VMEM(edge, f32),
            pltpu.VMEM(edge, f32),
            pltpu.VMEM((2, nz // BELOW, ny, nx), f32),
            pltpu.VMEM((2, 3, nz, ROWS, nx), f32),
            pltpu.VMEM((2, 3, depth, ROWS, nx), f32),
            pltpu.VMEM((3,) + wide, f32),
            pltpu.VMEM(wide, f32),
            pltpu.VMEM(wide, f32),
            pltpu.VMEM((3,) + wide, f32),
            pltpu.VMEM((3,) + wide, f32),
            pltpu.VMEM((3,) + wide, f32),
            pltpu.VMEM((3,) + wide, f32),
            pltpu.VMEM((3,) + wide, f32),
            pltpu.VMEM((3, pz, ny + ROWS, 2 * nx), f32),
            pltpu.VMEM((pz, py, px), f32),
            pltpu.VMEM((pz, py, px), f32),
            pltpu.VMEM(pressure_all, f32),
            pltpu.VMEM(pressure_all, f32),
            pltpu.VMEM((2, py, 2 * px), f32),
            pltpu.VMEM((2, 2, 3, py + 2 * ROWS, 2 * px), f32),
            pltpu.VMEM((2, 2 * nx, 2 * px), f32),
            pltpu.VMEM((pz, ny + ROWS, 2 * px), f32),
            pltpu.VMEM((3, nz, ny, nx), f32),
            pltpu.VMEM((pz, py, px), f32),
            pltpu.SemaphoreType.DMA((8,)),
            pltpu.SemaphoreType.DMA((4, ways)),
            pltpu.SemaphoreType.DMA((4, ways)),
        ],
        compiler_params=pltpu.CompilerParams(collective_id=0, has_side_effects=True),
    )(vrhs, prhs, visc, mass, pscale, vbounds, pbounds)


def solution(mesh):
    cells = P("gz", "gy", "gx")
    in_specs = (P(None, "gz", "gy", "gx"), cells, cells, cells, cells, P(), P())
    out_specs = (P(None, "gz", "gy", "gx"), cells)
    return jax.shard_map(
        per_device, mesh=mesh, in_specs=in_specs, out_specs=out_specs, check_vma=False
    )
```
